8 devices in a mesh: col: 2 (over z, y), row: 4 (over x, core).
Axes of the slice: x: 2, y: 2, z: 1, core: 2. Of those that a mesh axis runs over, the one named last changes fastest.
Arguments:
- adjacency: bfloat16 [8192, 8192], P('row', 'col')
- pers_vec: float32 [8192, 8], P(('row', 'col'))
- restart_wt: float32 [32, 8], replicated
Outputs:
- output 1: float32 [8192, 8], P(('col', 'row'))
- output 2: float32 [8192, 8], P(('row', 'col'))
All inputs are finite; a program needn't handle non-finite values.
Results may differ from the reference program's by a relative error of at most 0.001.
Values are sent between devices in bfloat16 or wider.
A program may use at most 1 GiB of HBM per device.

```python
import jax
import jax.numpy as jnp
from jax import lax

N = 8192
DEG = 15
M = 8
SWEEPS = 32


def setup_inputs(seed: int = 0) -> dict:
    base_key = jax.random.key(seed)
    k_out, k_pop, k_adj, k_start, k_val, k_rest = jax.random.split(base_key, 6)
    out_budget = jax.random.randint(k_out, (N,), 1, 2 * DEG + 1)
    popularity = jax.random.randint(k_pop, (N,), 1, 16)
    row_count = N // 16

    def draw_rows(block_idx):
        draw_bits = jax.random.randint(jax.random.fold_in(k_adj, block_idx), (row_count, N), 0, 8 * N)
        pop_rows = lax.dynamic_slice(popularity, (block_idx * row_count,), (row_count,))
        return (draw_bits < pop_rows[:, None] * out_budget[None, :]).astype(jnp.bfloat16)

    adjacency = lax.map(draw_rows, jnp.arange(16)).reshape(N, N)
    win_start = jax.random.randint(k_start, (M,), 0, N)
    inside = ((jnp.arange(N)[:, None] - win_start[None, :]) % N) < (N // 8)
    raw_vals = jnp.abs(jax.random.normal(k_val, (N, M), jnp.float32)) * jnp.where(inside, 1.0, 0.05)
    pers_vec = raw_vals * lax.rsqrt(jnp.mean(raw_vals * raw_vals, axis=0, keepdims=True))
    restart_wt = jax.random.uniform(k_rest, (SWEEPS, M), jnp.float32, 0.15, 0.45)
    return {"adjacency": adjacency, "pers_vec": pers_vec, "restart_wt": restart_wt}


def col_normalise(vals):
    return vals * lax.rsqrt(jnp.mean(vals * vals, axis=0, keepdims=True))


def reference(adjacency, pers_vec, restart_wt):
    def sweep(carry, weight):
        hub_vec = carry[0]
        auth_prod = lax.dot_general(adjacency, hub_vec.astype(jnp.bfloat16), (((0,), (0,)), ((), ())), preferred_element_type=jnp.float32)
        auth_vec = col_normalise(auth_prod)
        hub_prod = jnp.dot(adjacency, auth_vec.astype(jnp.bfloat16), preferred_element_type=jnp.float32)
        hub_new = (1.0 - weight) * col_normalise(hub_prod) + weight * pers_vec
        return (hub_new, auth_vec), None

    final_state, unused_out = lax.scan(sweep, (pers_vec, jnp.zeros_like(pers_vec)), restart_wt)
    return final_state[1], final_state[0]
```

```python
import functools

import jax
import jax.numpy as jnp
from jax import lax
from jax.experimental import pallas as pl
from jax.experimental.pallas import tpu as pltpu
from jax.sharding import PartitionSpec as P

MESH = pl.DeviceIdType.MESH
CHUNK = 512
STRIP = 256


def hits_kernel(a_ref, v_ref, b_ref, aout_ref, hout_ref, w1, w2, strips, vbuf, bbuf, xbuf, abuf, hbuf,
                s1, r1, d1s, d1r, s2, r2, d2s, d2r,
                strip_sem, own_sem, adj_sems, v_send, v_recv, send1, recv1, send2, recv2, dsend, drecv):
    rows, cols = a_ref.shape
    m = v_ref.shape[0]
    piece = v_ref.shape[1]
    half = s1.shape[1]
    sweeps = b_ref.shape[1]
    n_total = 4 * rows
    i = lax.axis_index("row")
    j = lax.axis_index("col")
    x = i // 2
    c = i % 2
    q1 = (c + x) % 2

    def dev(dx, dy, dc):
        return {"row": ((x + dx) % 2) * 2 + (c + dc) % 2, "col": (j + dy) % 2}

    def remote(src, dst, send, recv, where):
        return pltpu.make_async_remote_copy(src, dst, send, recv, device_id=where, device_id_type=MESH)

    n_strips = rows // STRIP

    def strip_copy(s, slot):
        return pltpu.make_async_copy(a_ref.at[pl.ds(s * STRIP, STRIP), :], strips.at[slot], strip_sem.at[slot])

    strip_copy(0, 0).start()
    own_half = pl.ds(pl.multiple_of(q1 * half, half), half)
    peer_half = pl.ds(pl.multiple_of((1 - q1) * half, half), half)
    own_rows = pl.ds(pl.multiple_of(c * rows, rows), rows)
    own_copy = pltpu.make_async_copy(a_ref.at[:, own_half], w1.at[own_rows, :], own_sem)

    barrier = pltpu.get_barrier_semaphore()
    for dx in range(2):
        for dy in range(2):
            for dc in range(2):
                if dx + dy + dc:
                    pl.semaphore_signal(barrier, inc=1, device_id=dev(dx, dy, dc), device_id_type=MESH)
    pl.semaphore_wait(barrier, 7)

    adj_copy = remote(a_ref.at[:, peer_half], w1.at[own_rows, :], adj_sems.at[0], adj_sems.at[1], dev(0, 0, 1))
    adj_copy.start()
    own_copy.start()
    my_v = vbuf.at[c * 2 + j]
    v_copies = []
    for n, (dy, dc) in enumerate(((0, 1), (1, 0), (1, 1))):
        copy = remote(v_ref, my_v, v_send.at[n], v_recv.at[n], dev(0, dy, dc))
        copy.start()
        v_copies.append(copy)
    my_v[...] = v_ref[...]
    b_cols = b_ref[...]
    for k in range(sweeps):
        bbuf[k] = jnp.broadcast_to(b_cols[:, k:k + 1], (m, 128))

    def strip_body(s, carry):
        slot = lax.rem(s, 2)

        @pl.when(s + 1 < n_strips)
        def _():
            strip_copy(s + 1, 1 - slot).start()

        strip_copy(s, slot).wait()
        w2[:, pl.ds(pl.multiple_of(s * STRIP, STRIP), STRIP)] = strips[slot].T
        return carry

    lax.fori_loop(0, n_strips, strip_body, 0)

    for copy in v_copies:
        copy.wait()
    for p in range(4):
        xbuf[:, p * piece:(p + 1) * piece] = vbuf[p].astype(jnp.bfloat16)
    own_copy.wait()
    adj_copy.wait()

    peers1 = (dev(1, 0, 1), dev(0, 1, 0), dev(1, 1, 1))
    peers2 = (dev(0, 1, 0), dev(1, 0, 0), dev(1, 1, 0))
    partner = dev(0, 0, 1)

    def product(w, s_buf, r_buf, send, recv, peers):
        for n in range(0, half, CHUNK):
            cut = slice(n, n + CHUNK)
            s_buf[:, cut] = jnp.dot(xbuf[...], w[:, cut], preferred_element_type=jnp.float32)
            for p in range(3):
                remote(s_buf.at[:, cut], r_buf.at[p, :, cut], send.at[p], recv.at[p], peers[p]).start()

    def reduce_and_swap(s_buf, r_buf, send, recv, peers, ds_buf, dr_buf, d):
        for p in range(3):
            remote(s_buf, r_buf.at[p], send.at[p], recv.at[p], peers[p]).wait_recv()
        sq = jnp.zeros((m, 128), jnp.float32)
        for n in range(0, half, 128):
            cut = slice(n, n + 128)
            own = s_buf[:, cut] + r_buf[0, :, cut]
            other = r_buf[1, :, cut] + r_buf[2, :, cut]
            ds_buf[:, cut] = own
            sq = sq + (own * own + other * other)
        ds_buf[:, half:] = sq
        swap = remote(ds_buf, dr_buf, dsend.at[d], drecv.at[d], partner)
        swap.start()
        for p in range(3):
            remote(s_buf, r_buf.at[p], send.at[p], recv.at[p], peers[p]).wait_send()
        swap.wait()
        total = jnp.sum(ds_buf[:, half:] + dr_buf[:, half:], axis=1, keepdims=True)
        return lax.rsqrt(total / n_total)

    def sweep(k, carry):
        product(w1, s1, r1, send1, recv1, peers1)
        scale = reduce_and_swap(s1, r1, send1, recv1, peers1, d1s, d1r, 0)
        a_own = d1s[:, :half] * scale
        a_peer = d1r[:, :half] * scale
        abuf[:, own_half] = a_own
        abuf[:, peer_half] = a_peer
        xbuf[:, own_half] = a_own.astype(jnp.bfloat16)
        xbuf[:, peer_half] = a_peer.astype(jnp.bfloat16)

        product(w2, s2, r2, send2, recv2, peers2)
        scale = reduce_and_swap(s2, r2, send2, recv2, peers2, d2s, d2r, 1)
        weight = bbuf[k]
        for buf, block, mine in ((d2s, c, True), (d2r, 1 - c, False)):
            for n in range(0, half, 128):
                v_piece = vbuf[block * 2 + n // piece, :, n % piece:n % piece + 128]
                h = (1.0 - weight) * (buf[:, n:n + 128] * scale) + weight * v_piece
                if mine:
                    hbuf[:, n:n + 128] = h
                xbuf[:, pl.ds(pl.multiple_of(block * half + n, 128), 128)] = h.astype(jnp.bfloat16)
        return carry

    lax.fori_loop(0, sweeps, sweep, 0)
    aout_ref[...] = abuf[:, pl.ds(pl.multiple_of(i * piece, piece), piece)]
    hout_ref[...] = hbuf[:, pl.ds(pl.multiple_of(j * piece, piece), piece)]


def solution(mesh):
    def device_fn(adj_tile, pers_piece, restart_wt):
        rows, cols = adj_tile.shape
        piece, m = pers_piece.shape
        half = cols // 2
        f32, bf16 = jnp.float32, jnp.bfloat16
        vmem = pl.BlockSpec(memory_space=pltpu.VMEM)
        exchange = [pltpu.VMEM((m, half), f32), pltpu.VMEM((3, m, half), f32),
                    pltpu.VMEM((m, half + 128), f32), pltpu.VMEM((m, half + 128), f32)]
        dma = pltpu.SemaphoreType.DMA
        auth_t, hub_t = pl.pallas_call(
            hits_kernel,
            out_shape=(jax.ShapeDtypeStruct((m, piece), f32), jax.ShapeDtypeStruct((m, piece), f32)),
            in_specs=[pl.BlockSpec(memory_space=pl.ANY), vmem, vmem],
            out_specs=(vmem, vmem),
            scratch_shapes=[
                pltpu.VMEM((2 * rows, half), bf16),
                pltpu.VMEM((cols, rows), bf16),
                pltpu.VMEM((2, STRIP, cols), bf16),
                pltpu.VMEM((4, m, piece), f32),
                pltpu.VMEM((restart_wt.shape[0], m, 128), f32),
                pltpu.VMEM((m, cols), bf16),
                pltpu.VMEM((m, cols), f32),
                pltpu.VMEM((m, half), f32),
                *exchange, *exchange,
                dma((2,)), dma, dma((2,)), dma((3,)), dma((3,)),
                dma((3,)), dma((3,)), dma((3,)), dma((3,)), dma((2,)), dma((2,)),
            ],
            compiler_params=pltpu.CompilerParams(collective_id=0, has_side_effects=True, vmem_limit_bytes=58 * 2**20),
        )(adj_tile, pers_piece.T, restart_wt.T)
        return auth_t.T, hub_t.T

    return jax.shard_map(device_fn, mesh=mesh, in_specs=(P("row", "col"), P(("row", "col"), None), P(None, None)), out_specs=(P(("col", "row"), None), P(("row", "col"), None)), check_vma=False)
```
